128 devices in a mesh: grp: 16 (over z, y), blk: 8 (over x, core).
Axes of the slice: x: 4, y: 4, z: 4, core: 2. Of those that a mesh axis runs over, the one named last changes fastest.
Arguments:
- queries: bfloat16 [81920, 2048], P(('grp', 'blk')), may hold values from -6 to 6
- key_rows: bfloat16 [81920, 256], P(('grp', 'blk')), may hold values from -6 to 6
- value_rows: bfloat16 [81920, 256], P(('grp', 'blk')), may hold values from -6 to 6
- out_grad: bfloat16 [81920, 2048], P(('grp', 'blk')), may hold values from -12 to 12
- attn_out: bfloat16 [81920, 2048], P(('grp', 'blk')), may hold values from -6 to 6
- log_norm: float32 [81920, 16], P(('grp', 'blk')), may hold values from 4 to 7
- held_block: int32 [128], replicated, may hold values from 0 to 127, as said below
- key_block: int32 [128], replicated, may hold values from 0 to 127, as said below
Outputs:
- query_grad: bfloat16 [81920, 2048], P(('grp', 'blk'))
- key_grad: bfloat16 [81920, 256], P(('grp', 'blk'))
- value_grad: bfloat16 [81920, 256], P(('grp', 'blk'))
The draws below stay inside these ranges and needn't reach their ends.
Inputs may be any that keep to these rules, and one draw needn't show every extreme that they name: held_block is a permutation of the 128 blocks. key_block[d] <= held_block[d] for every d; a key block may be paired with many query blocks or none.
All inputs are finite; a program needn't handle non-finite values.
Results may differ from the reference program's by a relative error of at most 0.0069.
Values may be sent and summed in bfloat16 or wider, within the bound.
No kernel may reach another device: no remote copies, remote signals or barrier semaphores. Data moves between devices by JAX's collectives and lax.ppermute only.
A program may use at most 192 MiB of HBM per device.

```python
import jax
import jax.numpy as jnp
from jax import lax

H = 16
KVH = 2
DH = 128
BLK = 640
BLOCKS = 128


def plan_pair(key):
    held = jax.random.permutation(jax.random.fold_in(key, 11), BLOCKS).astype(jnp.int32)
    raw = jax.random.randint(jax.random.fold_in(key, 12), (BLOCKS,), 0, 1048576, dtype=jnp.int32)
    chosen = raw % (held + 1)
    chosen = jnp.where(held == BLOCKS - 1, held, chosen)
    return (held, chosen.astype(jnp.int32))


def draw_held_block(key, part):
    return plan_pair(key)[0]


def draw_key_block(key, part):
    return plan_pair(key)[1]


def shard_levels(own_key, extent, split, low, high):
    level = 1.0
    for axis_at, parts in split:
        heights = jax.random.uniform(jax.random.fold_in(jax.random.fold_in(own_key, 6), axis_at), (parts,), jnp.float32, low / len(split), high / len(split))
        level = level * jnp.repeat(jnp.exp(heights), extent[axis_at] // parts).reshape((-1,) + (1,) * (len(extent) - 1 - axis_at))
    return level


def noise(rng, extent, scale, limit, pieces=(), kind=jnp.bfloat16):
    loudness = shard_levels(rng, extent, pieces, -0.22, 0.18) if pieces else 1.0
    result = jax.random.normal(rng, extent, jnp.float32) * scale * loudness
    return jnp.minimum(jnp.maximum(result, -limit), limit).astype(kind)


def setup_inputs(seed: int = 0) -> dict:
    streams_of = jax.random.split(jax.random.key(seed), 9)
    queries = noise(streams_of[0], (BLOCKS * BLK, H * DH), 1.0, 6.0, ((0, 128),))
    key_rows = noise(streams_of[1], (BLOCKS * BLK, KVH * DH), 1.0, 6.0, ((0, 128),))
    value_rows = noise(streams_of[2], (BLOCKS * BLK, KVH * DH), 1.0, 6.0, ((0, 128),))
    out_grad = noise(streams_of[3], (BLOCKS * BLK, H * DH), 2.0, 12.0, ((0, 128),))
    attn_out = noise(streams_of[4], (BLOCKS * BLK, H * DH), 1.0, 6.0, ((0, 128),))
    log_norm = jnp.clip(4.0 + 3.0 * jax.random.uniform(streams_of[5], (BLOCKS * BLK, H), jnp.float32) ** shard_levels(streams_of[5], (BLOCKS * BLK, H), ((0, 128),), -0.2, 0.2), 4.0, 7.0)
    held_block = draw_held_block(jax.random.fold_in(streams_of[8], 71), 0)
    key_block = draw_key_block(jax.random.fold_in(streams_of[8], 71), 0)
    return dict(queries=queries, key_rows=key_rows, value_rows=value_rows, out_grad=out_grad, attn_out=attn_out, log_norm=log_norm, held_block=held_block, key_block=key_block)


def pair_grads(query, dout, outs, norms, kv_rows, diag):
    rows = query.shape[0]
    group = H // KVH
    scale = DH ** -0.5
    delta = jnp.sum((dout.astype(jnp.float32) * outs.astype(jnp.float32)).reshape(rows, H, DH), axis=-1)
    row_ids = lax.broadcasted_iota(jnp.int32, (rows, rows), 0)
    col_ids = lax.broadcasted_iota(jnp.int32, (rows, rows), 1)
    keep = jnp.logical_or(jnp.logical_not(diag), col_ids <= row_ids)
    query_parts, key_parts, value_parts = [], [], []
    for head in range(KVH):
        width = group * DH
        q_head = query[:, head * width:(head + 1) * width].reshape(rows, group, DH)
        o_head = dout[:, head * width:(head + 1) * width].reshape(rows, group, DH)
        k_head = kv_rows[:, head * DH:(head + 1) * DH]
        v_head = kv_rows[:, (KVH + head) * DH:(KVH + head + 1) * DH]
        scores = jnp.einsum("igd,jd->gij", q_head.astype(jnp.float32), k_head.astype(jnp.float32)) * scale
        lse_head = jnp.transpose(norms[:, head * group:(head + 1) * group])[:, :, None]
        probs = jnp.where(keep[None], jnp.exp(scores - lse_head), 0.0)
        probs_low = probs.astype(jnp.bfloat16)
        dv_head = jnp.einsum("gij,igd->jd", probs_low.astype(jnp.float32), o_head.astype(jnp.float32))
        dprob = jnp.einsum("igd,jd->gij", o_head.astype(jnp.float32), v_head.astype(jnp.float32))
        delta_head = jnp.transpose(delta[:, head * group:(head + 1) * group])[:, :, None]
        dscore = (probs * (dprob - delta_head) * scale).astype(jnp.bfloat16)
        dq_head = jnp.einsum("gij,jd->igd", dscore.astype(jnp.float32), k_head.astype(jnp.float32))
        dk_head = jnp.einsum("gij,igd->jd", dscore.astype(jnp.float32), q_head.astype(jnp.float32))
        query_parts.append(dq_head.reshape(rows, width))
        key_parts.append(dk_head)
        value_parts.append(dv_head)
    query_grad = jnp.concatenate(query_parts, axis=1).astype(jnp.bfloat16)
    pair_term = jnp.concatenate(key_parts + value_parts, axis=1).astype(jnp.bfloat16)
    return query_grad, pair_term


def reference(queries, key_rows, value_rows, out_grad, attn_out, log_norm, held_block, key_block):
    count = held_block.shape[0]
    positions = jnp.arange(count, dtype=jnp.int32)
    holder = jnp.sum(jnp.where(held_block[None, :] == key_block[:, None], positions[None, :], 0), axis=1).astype(jnp.int32)
    q_all = queries.reshape(count, BLK, H * DH)
    d_all = out_grad.reshape(count, BLK, H * DH)
    o_all = attn_out.reshape(count, BLK, H * DH)
    n_all = log_norm.reshape(count, BLK, H)
    kv_all = jnp.concatenate([key_rows, value_rows], axis=1).reshape(count, BLK, 2 * KVH * DH)

    def one(index):
        kv_rows = kv_all[holder[index]]
        diag = held_block[index] == key_block[index]
        return pair_grads(q_all[index], d_all[index], o_all[index], n_all[index], kv_rows, diag)

    query_grad, pair_terms = lax.map(one, positions)
    summed = jax.ops.segment_sum(pair_terms.astype(jnp.float32), holder, num_segments=count)
    summed = summed.reshape(count * BLK, 2 * KVH * DH).astype(jnp.bfloat16)
    return (query_grad.reshape(count * BLK, H * DH), summed[:, :KVH * DH], summed[:, KVH * DH:])
```

```python
import functools

import jax
import jax.numpy as jnp
from jax import lax
from jax.experimental import pallas as pl
from jax.experimental.pallas import tpu as pltpu
from jax.sharding import PartitionSpec as P

H = 16
KVH = 2
DH = 128
GROUP = H // KVH
AXES = ("grp", "blk")
SCALE = DH ** (-0.5)
LOG2E = 1.4426950408889634
STEP_HEADS = 2


def spread_kernel(k_ref, v_ref, out_ref):
    parts = out_ref.shape[0]
    depth = out_ref.shape[1]
    half = parts // 2
    for at, ref in enumerate((k_ref, v_ref)):
        turned = ref[...].T
        out_ref[at * half : (at + 1) * half] = turned.reshape(half, depth, turned.shape[1])


def fill_positions(held_ref, pos_ref):
    def put(e, carry):
        pos_ref[held_ref[e]] = e
        return carry

    lax.fori_loop(0, held_ref.shape[0], put, 0, unroll=8)


def select_kernel(held_ref, key_ref, in_ref, out_ref, pos_ref):
    fill_positions(held_ref, pos_ref)

    def move(d, carry):
        out_ref[d] = in_ref[pos_ref[key_ref[d]]]
        return carry

    lax.fori_loop(0, key_ref.shape[0], move, 0, unroll=8)


def pool_kernel(held_ref, key_ref, in_ref, out_ref, pos_ref, total_ref):
    fill_positions(held_ref, pos_ref)
    total_ref[...] = jnp.zeros_like(total_ref)

    def add(d, carry):
        at = pos_ref[key_ref[d]]
        total_ref[at] = total_ref[at] + in_ref[d].astype(jnp.float32)
        return carry

    lax.fori_loop(0, key_ref.shape[0], add, 0, unroll=8)
    out_ref[...] = total_ref[...].astype(out_ref.dtype)


def finish_kernel(in_ref, k_ref, v_ref):
    parts, depth, rows = in_ref.shape
    half = parts // 2
    for at, ref in enumerate((k_ref, v_ref)):
        flat = in_ref[at * half : (at + 1) * half].reshape(half * depth, rows)
        ref[...] = flat.T


def pair_kernel(
    off_ref, q_ref, do_ref, o_ref, norm_ref, kv_ref, dq_ref, term_ref,
    flat_ref, k_ref, dk_ref, dv_ref,
):
    step = pl.program_id(0)
    per_group = GROUP // STEP_HEADS
    c = step // per_group
    at = step % per_group
    rows = q_ref.shape[0]
    depth = kv_ref.shape[1]
    pieces = DH // depth

    @pl.when(step == 0)
    def _():
        flat_ref[...] = kv_ref[...].reshape(flat_ref.shape)

    @pl.when(at == 0)
    def _():
        k_ref[...] = flat_ref[pl.ds(pl.multiple_of(c * DH, DH), DH), :].T
        dk_ref[...] = jnp.zeros_like(dk_ref)
        dv_ref[...] = jnp.zeros_like(dv_ref)

    k_t = flat_ref[pl.ds(pl.multiple_of(c * DH, DH), DH), :]
    v_t = flat_ref[pl.ds(pl.multiple_of((KVH + c) * DH, DH), DH), :]
    k_rows = k_ref[...]
    limit = lax.broadcasted_iota(jnp.int32, (rows, 1), 0) + off_ref[0]
    keep = lax.broadcasted_iota(jnp.int32, (rows, rows), 1) <= limit
    norms = norm_ref[...]
    lanes = lax.broadcasted_iota(jnp.int32, norms.shape, 1)
    dk = dk_ref[...]
    dv = dv_ref[...]
    for sub in range(STEP_HEADS):
        cols = slice(sub * DH, (sub + 1) * DH)
        q = q_ref[:, cols]
        do = do_ref[:, cols]
        delta = jnp.sum(
            do.astype(jnp.float32) * o_ref[:, cols].astype(jnp.float32), axis=1, keepdims=True
        )
        lse = jnp.sum(
            jnp.where(lanes == step * STEP_HEADS + sub, norms, 0.0), axis=1, keepdims=True
        )
        s = jnp.dot(q, k_t, preferred_element_type=jnp.float32)
        dp = jnp.dot(do, v_t, preferred_element_type=jnp.float32)
        p = jnp.exp2(jnp.where(keep, s * (SCALE * LOG2E) - lse * LOG2E, -jnp.inf))
        ds = (p * (dp - delta)).astype(jnp.bfloat16)
        dq = jnp.dot(ds, k_rows, preferred_element_type=jnp.float32) * SCALE
        dq_ref[:, cols] = dq.astype(dq_ref.dtype)
        dv = dv + jnp.dot(do.T, p.astype(jnp.bfloat16), preferred_element_type=jnp.float32)
        dk = dk + jnp.dot(q.T, ds, preferred_element_type=jnp.float32)
    dk_ref[...] = dk
    dv_ref[...] = dv

    @pl.when(at == per_group - 1)
    def _():
        low_k = (dk_ref[...] * SCALE).astype(term_ref.dtype)
        low_v = dv_ref[...].astype(term_ref.dtype)
        term_ref[pl.ds(c * pieces, pieces)] = low_k.reshape(pieces, depth, rows)
        term_ref[pl.ds((KVH + c) * pieces, pieces)] = low_v.reshape(pieces, depth, rows)


def exchange(x):
    return lax.all_to_all(x, AXES, split_axis=0, concat_axis=0, tiled=True)


def per_device(queries, key_rows, value_rows, out_grad, attn_out, log_norm, held_block, key_block):
    count = lax.axis_size("grp") * lax.axis_size("blk")
    own = lax.axis_index("grp") * lax.axis_size("blk") + lax.axis_index("blk")
    rows = queries.shape[0]
    depth = 2 * KVH * DH // count
    piece = (count, depth, rows)
    low = jax.ShapeDtypeStruct(piece, jnp.bfloat16)
    vmem = pl.BlockSpec(memory_space=pltpu.VMEM)
    smem = pl.BlockSpec(memory_space=pltpu.SMEM)

    spread = pl.pallas_call(
        spread_kernel, out_shape=low, in_specs=[vmem] * 2, out_specs=vmem, name="spread"
    )(key_rows, value_rows)
    gathered = exchange(spread)
    chosen = pl.pallas_call(
        select_kernel,
        out_shape=low,
        in_specs=[smem, smem, vmem],
        out_specs=vmem,
        scratch_shapes=[pltpu.SMEM((count,), jnp.int32)],
        name="select",
    )(held_block, key_block, gathered)
    kv = exchange(chosen)

    own_query = lax.dynamic_index_in_dim(held_block, own, 0)
    own_key = lax.dynamic_index_in_dim(key_block, own, 0)
    off = jnp.where(own_query == own_key, 0, rows).astype(jnp.int32)
    width = STEP_HEADS * DH
    wide = pl.BlockSpec((rows, width), lambda s: (0, s))
    query_grad, term = pl.pallas_call(
        pair_kernel,
        grid=(H // STEP_HEADS,),
        out_shape=(jax.ShapeDtypeStruct(queries.shape, jnp.bfloat16), low),
        in_specs=[
            smem, wide, wide, wide,
            pl.BlockSpec(log_norm.shape, lambda s: (0, 0)),
            pl.BlockSpec(piece, lambda s: (0, 0, 0)),
        ],
        out_specs=(wide, pl.BlockSpec(piece, lambda s: (0, 0, 0))),
        scratch_shapes=[
            pltpu.VMEM((2 * KVH * DH, rows), jnp.bfloat16),
            pltpu.VMEM((rows, DH), jnp.bfloat16),
            pltpu.VMEM((DH, rows), jnp.float32),
            pltpu.VMEM((DH, rows), jnp.float32),
        ],
        compiler_params=pltpu.CompilerParams(
            dimension_semantics=("arbitrary",), vmem_limit_bytes=56 * 1024 * 1024
        ),
        name="pair",
    )(off, queries, out_grad, attn_out, log_norm, kv)

    returned = exchange(term)
    pooled = pl.pallas_call(
        pool_kernel,
        out_shape=low,
        in_specs=[smem, smem, vmem],
        out_specs=vmem,
        scratch_shapes=[pltpu.SMEM((count,), jnp.int32), pltpu.VMEM(piece, jnp.float32)],
        name="pool",
    )(held_block, key_block, returned)
    home = exchange(pooled)
    key_grad, value_grad = pl.pallas_call(
        finish_kernel,
        out_shape=(
            jax.ShapeDtypeStruct(key_rows.shape, jnp.bfloat16),
            jax.ShapeDtypeStruct(value_rows.shape, jnp.bfloat16),
        ),
        in_specs=[vmem],
        out_specs=(vmem, vmem),
        name="finish",
    )(home)
    return (query_grad, key_grad, value_grad)


def solution(mesh):
    rows = P(AXES, None)
    return jax.shard_map(
        per_device,
        mesh=mesh,
        in_specs=(rows,) * 6 + (P(), P()),
        out_specs=(rows, rows, rows),
        check_vma=False,
    )
```

```python
import functools

import jax
import jax.numpy as jnp
from jax import lax
from jax.experimental import pallas as pl
from jax.experimental.pallas import tpu as pltpu
from jax.sharding import PartitionSpec as P

H = 16
KVH = 2
DH = 128
GROUP = H // KVH
AXES = ("grp", "blk")
SCALE = DH ** (-0.5)
LOG2E = 1.4426950408889634
STEP_HEADS = 2
TERMS = 3
SMALL = pltpu.CompilerParams(vmem_limit_bytes=8 * 1024 * 1024)
BIG_LIMIT = 125 * 512 * 1024
FULL_LIMIT = 67043328


def spread_kernel(k_hbm, v_hbm, out_ref, k_ref, v_ref, sems):
    parts, depth, rows = out_ref.shape
    half = parts // 2
    copies = [
        pltpu.make_async_copy(k_hbm, k_ref, sems.at[0]),
        pltpu.make_async_copy(v_hbm, v_ref, sems.at[1]),
    ]
    for copy in copies:
        copy.start()
    for at, ref in enumerate((k_ref, v_ref)):
        copies[at].wait()
        out_ref[at * half : (at + 1) * half] = ref[...].T.reshape(half, depth, rows)


def prep_kernel(
    own_ref, held_ref, key_ref, norm_ref, q_ref, do_ref, o_ref,
    holder_ref, off_ref, aux_ref, q_t_ref, do_t_ref, pos_ref, delta_ref,
):
    step = pl.program_id(0)
    rows = q_ref.shape[0]
    count = held_ref.shape[0]

    @pl.when(step == 0)
    def _():
        def put(e, carry):
            pos_ref[held_ref[e]] = e
            return carry

        def look(d, carry):
            holder_ref[d] = pos_ref[key_ref[d]]
            return carry

        lax.fori_loop(0, count, put, 0, unroll=8)
        lax.fori_loop(0, count, look, 0, unroll=8)
        own = own_ref[0]
        off_ref[0] = jnp.where(held_ref[own] == key_ref[own], 0, rows)
        delta_ref[...] = jnp.zeros_like(delta_ref)

    q_t_ref[...] = q_ref[...].T
    do_t_ref[...] = do_ref[...].T
    lanes = lax.broadcasted_iota(jnp.int32, delta_ref.shape, 1)
    delta = delta_ref[...]
    for sub in range(STEP_HEADS):
        cols = slice(sub * DH, (sub + 1) * DH)
        both = do_ref[:, cols].astype(jnp.float32) * o_ref[:, cols].astype(jnp.float32)
        one = jnp.sum(both, axis=1, keepdims=True)
        delta = jnp.where(lanes == step * STEP_HEADS + sub, one, delta)
    delta_ref[...] = delta

    @pl.when(step == pl.num_programs(0) - 1)
    def _():
        norms = norm_ref[...] * DH**0.5
        norms = jnp.concatenate([norms, jnp.zeros((rows, DH - H), jnp.float32)], axis=1)
        total = jnp.zeros((rows, DH), jnp.float32)
        for at, left in enumerate((norms, delta_ref[...])):
            for term in range(TERMS):
                part = left.astype(jnp.bfloat16).astype(jnp.float32)
                left = left - part
                shift = (at * TERMS + term) * H
                total = total + (pltpu.roll(part, shift, 1) if shift else part)
        aux_ref[...] = total.astype(aux_ref.dtype)


def select_kernel(holder_ref, in_ref, out_ref):
    def move(d, carry):
        out_ref[d] = in_ref[holder_ref[d]]
        return carry

    lax.fori_loop(0, holder_ref.shape[0], move, 0, unroll=8)


def pool_kernel(holder_ref, in_ref, out_ref, total_ref):
    total_ref[...] = jnp.zeros_like(total_ref)

    def add(d, carry):
        at = holder_ref[d]
        total_ref[at] = total_ref[at] + in_ref[d].astype(jnp.float32)
        return carry

    lax.fori_loop(0, holder_ref.shape[0], add, 0, unroll=8)
    out_ref[...] = total_ref[...].astype(out_ref.dtype)


def finish_kernel(in_ref, k_ref, v_ref):
    parts, depth, rows = in_ref.shape
    half = parts // 2
    for at, ref in enumerate((k_ref, v_ref)):
        flat = in_ref[at * half : (at + 1) * half].reshape(half * depth, rows)
        ref[...] = flat.T


def picker(which, head):
    row = lax.broadcasted_iota(jnp.int32, (DH, DH), 0) - which * TERMS * H
    hit = (row >= 0) & (row < TERMS * H) & (row % H == head)
    return jnp.where(hit, -1.0, 0.0).astype(jnp.bfloat16)


def pair_kernel(
    off_ref, q_ref, do_ref, q_t_ref, do_t_ref, aux_ref, kv_ref, ds_ref, term_ref,
    flat_ref, bias_ref, dk_ref, dv_ref,
):
    step = pl.program_id(0)
    per_group = GROUP // STEP_HEADS
    c = step // per_group
    at = step % per_group
    rows = q_ref.shape[0]
    depth = kv_ref.shape[1]
    pieces = DH // depth

    @pl.when(step == 0)
    def _():
        flat_ref[...] = kv_ref[...].reshape(flat_ref.shape)
        limit = lax.broadcasted_iota(jnp.int32, (rows, rows), 0) + off_ref[0]
        col = lax.broadcasted_iota(jnp.int32, (rows, rows), 1)
        bias_ref[...] = jnp.where(col <= limit, 0.0, -jnp.inf)

    @pl.when(at == 0)
    def _():
        dk_ref[...] = jnp.zeros_like(dk_ref)
        dv_ref[...] = jnp.zeros_like(dv_ref)

    k_t = flat_ref[pl.ds(pl.multiple_of(c * DH, DH), DH), :]
    v_t = flat_ref[pl.ds(pl.multiple_of((KVH + c) * DH, DH), DH), :]
    aux = aux_ref[...]

    def shifted(left, right, which, head):
        tail = jnp.concatenate([picker(which, head)] * (rows // DH), axis=1)
        return jnp.dot(
            jnp.concatenate([left, aux], axis=1),
            jnp.concatenate([right, tail], axis=0),
            preferred_element_type=jnp.float32,
        )

    for sub in range(STEP_HEADS):
        cols = slice(sub * DH, (sub + 1) * DH)
        head = step * STEP_HEADS + sub
        s = shifted(q_ref[:, cols], k_t, 0, head)
        dp = shifted(do_ref[:, cols], v_t, 1, head)
        p = jnp.exp2(s * (DH**-0.5 * LOG2E) + bias_ref[...])
        ds = (p * dp).astype(jnp.bfloat16)
        ds_ref[sub] = ds
        dv_ref[...] += jnp.dot(
            do_t_ref[cols, :], p.astype(jnp.bfloat16), preferred_element_type=jnp.float32
        )
        dk_ref[...] += jnp.dot(q_t_ref[cols, :], ds, preferred_element_type=jnp.float32)

    @pl.when(at == per_group - 1)
    def _():
        low_k = (dk_ref[...] * SCALE).astype(term_ref.dtype)
        low_v = dv_ref[...].astype(term_ref.dtype)
        term_ref[pl.ds(c * pieces, pieces)] = low_k.reshape(pieces, depth, rows)
        term_ref[pl.ds((KVH + c) * pieces, pieces)] = low_v.reshape(pieces, depth, rows)


def query_kernel(ds_ref, kv_ref, dq_ref, flat_ref, k_ref):
    step = pl.program_id(0)
    per_group = GROUP // STEP_HEADS
    c = step // per_group

    @pl.when(step == 0)
    def _():
        flat_ref[...] = kv_ref[: kv_ref.shape[0] // 2].reshape(flat_ref.shape)

    @pl.when(step % per_group == 0)
    def _():
        k_ref[...] = flat_ref[pl.ds(pl.multiple_of(c * DH, DH), DH), :].T

    for sub in range(STEP_HEADS):
        dq = jnp.dot(ds_ref[sub], k_ref[...], preferred_element_type=jnp.float32) * SCALE
        dq_ref[:, sub * DH : (sub + 1) * DH] = dq.astype(dq_ref.dtype)


def exchange(x):
    return lax.all_to_all(x, AXES, split_axis=0, concat_axis=0, tiled=True)


def cost(flops, bytes_accessed):
    return pl.CostEstimate(flops=flops, bytes_accessed=bytes_accessed, transcendentals=0)


def per_device(queries, key_rows, value_rows, out_grad, attn_out, log_norm, held_block, key_block):
    count = lax.axis_size("grp") * lax.axis_size("blk")
    own = lax.axis_index("grp") * lax.axis_size("blk") + lax.axis_index("blk")
    rows = queries.shape[0]
    depth = 2 * KVH * DH // count
    piece = (count, depth, rows)
    low = jax.ShapeDtypeStruct(piece, jnp.bfloat16)
    vmem = pl.BlockSpec(memory_space=pltpu.VMEM)
    smem = pl.BlockSpec(memory_space=pltpu.SMEM)
    hbm = pl.BlockSpec(memory_space=pltpu.HBM)
    width = STEP_HEADS * DH
    steps = H // STEP_HEADS
    wide = pl.BlockSpec((rows, width), lambda s: (0, s))
    tall = pl.BlockSpec((width, rows), lambda s: (s, 0))
    whole = pl.BlockSpec(piece, lambda s: (0, 0, 0))
    aux_spec = pl.BlockSpec((rows, DH), lambda s: (0, 0))
    big = pltpu.CompilerParams(
        dimension_semantics=("arbitrary",), vmem_limit_bytes=BIG_LIMIT
    )
    matmul = 2 * H * rows * rows * DH
    wide_bytes = 2 * rows * H * DH

    spread = pl.pallas_call(
        spread_kernel,
        out_shape=low,
        in_specs=[hbm] * 2,
        out_specs=vmem,
        scratch_shapes=[
            pltpu.VMEM(key_rows.shape, jnp.bfloat16),
            pltpu.VMEM(value_rows.shape, jnp.bfloat16),
            pltpu.SemaphoreType.DMA((2,)),
        ],
        compiler_params=pltpu.CompilerParams(vmem_limit_bytes=FULL_LIMIT),
        name="spread",
    )(key_rows, value_rows)
    gathered = exchange(spread)
    turned = jax.ShapeDtypeStruct((H * DH, rows), jnp.bfloat16)
    holder, off, aux, q_t, do_t = pl.pallas_call(
        prep_kernel,
        grid=(steps,),
        out_shape=(
            jax.ShapeDtypeStruct((count,), jnp.int32),
            jax.ShapeDtypeStruct((1,), jnp.int32),
            jax.ShapeDtypeStruct((rows, DH), jnp.bfloat16),
            turned,
            turned,
        ),
        in_specs=[
            smem, smem, smem, pl.BlockSpec(log_norm.shape, lambda s: (0, 0)), wide, wide, wide,
        ],
        out_specs=(smem, smem, aux_spec, tall, tall),
        scratch_shapes=[pltpu.SMEM((count,), jnp.int32), pltpu.VMEM((rows, DH), jnp.float32)],
        compiler_params=big,
        cost_estimate=cost(matmul // 2, 5 * wide_bytes),
        name="prep",
    )(own.reshape(1).astype(jnp.int32), held_block, key_block, log_norm, queries, out_grad, attn_out)
    chosen = pl.pallas_call(
        select_kernel,
        out_shape=low,
        in_specs=[smem, vmem],
        out_specs=vmem,
        compiler_params=SMALL,
        name="select",
    )(holder, gathered)
    kv = exchange(chosen)

    kept = pl.BlockSpec((STEP_HEADS, rows, rows), lambda s: (s, 0, 0))
    ds, term = pl.pallas_call(
        pair_kernel,
        grid=(steps,),
        out_shape=(jax.ShapeDtypeStruct((H, rows, rows), jnp.bfloat16), low),
        in_specs=[smem, wide, wide, tall, tall, aux_spec, whole],
        out_specs=(kept, whole),
        scratch_shapes=[
            pltpu.VMEM((2 * KVH * DH, rows), jnp.bfloat16),
            pltpu.VMEM((rows, rows), jnp.float32),
            pltpu.VMEM((DH, rows), jnp.float32),
            pltpu.VMEM((DH, rows), jnp.float32),
        ],
        compiler_params=big,
        cost_estimate=cost(4 * matmul, 4 * wide_bytes + 2 * H * rows * rows),
        name="pair",
    )(off, queries, out_grad, q_t, do_t, aux, kv)
    returned = exchange(term)
    query_grad = pl.pallas_call(
        query_kernel,
        grid=(steps,),
        out_shape=jax.ShapeDtypeStruct(queries.shape, jnp.bfloat16),
        in_specs=[kept, whole],
        out_specs=wide,
        scratch_shapes=[
            pltpu.VMEM((KVH * DH, rows), jnp.bfloat16),
            pltpu.VMEM((rows, DH), jnp.bfloat16),
        ],
        compiler_params=big,
        cost_estimate=cost(matmul, wide_bytes + 2 * H * rows * rows),
        name="query",
    )(ds, kv)
    pooled = pl.pallas_call(
        pool_kernel,
        out_shape=low,
        in_specs=[smem, vmem],
        out_specs=vmem,
        scratch_shapes=[pltpu.VMEM(piece, jnp.float32)],
        compiler_params=SMALL,
        name="pool",
    )(holder, returned)
    home = exchange(pooled)
    key_grad, value_grad = pl.pallas_call(
        finish_kernel,
        out_shape=(
            jax.ShapeDtypeStruct(key_rows.shape, jnp.bfloat16),
            jax.ShapeDtypeStruct(value_rows.shape, jnp.bfloat16),
        ),
        in_specs=[vmem],
        out_specs=(vmem, vmem),
        compiler_params=SMALL,
        name="finish",
    )(home)
    return (query_grad, key_grad, value_grad)


def solution(mesh):
    rows = P(AXES, None)
    return jax.shard_map(
        per_device,
        mesh=mesh,
        in_specs=(rows,) * 6 + (P(), P()),
        out_specs=(rows, rows, rows),
        check_vma=False,
    )
```

```python
import functools

import jax
import jax.numpy as jnp
from jax import lax
from jax.experimental import pallas as pl
from jax.experimental.pallas import tpu as pltpu
from jax.sharding import PartitionSpec as P

H = 16
KVH = 2
DH = 128
GROUP = H // KVH
AXES = ("grp", "blk")
SCALE = DH ** (-0.5)
LOG2E = 1.4426950408889634
STEP_HEADS = 4
TERMS = 3
SMALL = pltpu.CompilerParams(vmem_limit_bytes=8 * 1024 * 1024)
BLOCK = 640
BIG_LIMIT = 125 * 512 * 1024
FULL_LIMIT = 67043328


def spread_kernel(k_hbm, v_hbm, out_ref, k_ref, v_ref, sems):
    parts, depth, rows = out_ref.shape
    half = parts // 2
    copies = [
        pltpu.make_async_copy(k_hbm, k_ref, sems.at[0]),
        pltpu.make_async_copy(v_hbm, v_ref, sems.at[1]),
    ]
    for copy in copies:
        copy.start()
    for at, ref in enumerate((k_ref, v_ref)):
        copies[at].wait()
        out_ref[at * half : (at + 1) * half] = ref[...].T.reshape(half, depth, rows)


def table_kernel(own_ref, held_ref, key_ref, holder_ref, off_ref, pos_ref):
    def put(e, carry):
        pos_ref[held_ref[e]] = e
        return carry

    def look(d, carry):
        holder_ref[d] = pos_ref[key_ref[d]]
        return carry

    count = held_ref.shape[0]
    lax.fori_loop(0, count, put, 0, unroll=8)
    lax.fori_loop(0, count, look, 0, unroll=8)
    own = own_ref[0]
    off_ref[0] = jnp.where(held_ref[own] == key_ref[own], 0, BLOCK)


def prep_kernel(
    norm_ref, do_ref, o_ref, aux_ref, delta_ref,
):
    step = pl.program_id(0)
    rows = do_ref.shape[0]

    @pl.when(step == 0)
    def _():
        delta_ref[...] = jnp.zeros_like(delta_ref)

    lanes = lax.broadcasted_iota(jnp.int32, delta_ref.shape, 1)
    delta = delta_ref[...]
    for sub in range(STEP_HEADS):
        cols = slice(sub * DH, (sub + 1) * DH)
        both = do_ref[:, cols].astype(jnp.float32) * o_ref[:, cols].astype(jnp.float32)
        one = jnp.sum(both, axis=1, keepdims=True)
        delta = jnp.where(lanes == step * STEP_HEADS + sub, one, delta)
    delta_ref[...] = delta

    @pl.when(step == pl.num_programs(0) - 1)
    def _():
        norms = norm_ref[...] * DH**0.5
        norms = jnp.concatenate([norms, jnp.zeros((rows, DH - H), jnp.float32)], axis=1)
        total = jnp.zeros((rows, DH), jnp.float32)
        for at, left in enumerate((norms, delta_ref[...])):
            for term in range(TERMS):
                part = left.astype(jnp.bfloat16).astype(jnp.float32)
                left = left - part
                shift = (at * TERMS + term) * H
                total = total + (pltpu.roll(part, shift, 1) if shift else part)
        aux_ref[...] = total.astype(aux_ref.dtype)


def select_kernel(holder_ref, in_ref, out_ref):
    def move(d, carry):
        out_ref[d] = in_ref[holder_ref[d]]
        return carry

    lax.fori_loop(0, holder_ref.shape[0], move, 0, unroll=8)


def pool_kernel(holder_ref, in_ref, out_ref, total_ref):
    total_ref[...] = jnp.zeros_like(total_ref)

    def add(d, carry):
        at = holder_ref[d]
        total_ref[at] = total_ref[at] + in_ref[d].astype(jnp.float32)
        return carry

    lax.fori_loop(0, holder_ref.shape[0], add, 0, unroll=8)
    out_ref[...] = total_ref[...].astype(out_ref.dtype)


def finish_kernel(in_ref, k_ref, v_ref):
    parts, depth, rows = in_ref.shape
    half = parts // 2
    for at, ref in enumerate((k_ref, v_ref)):
        flat = in_ref[at * half : (at + 1) * half].reshape(half * depth, rows)
        ref[...] = flat.T


def picker(which, head):
    row = lax.broadcasted_iota(jnp.int32, (DH, DH), 0) - which * TERMS * H
    hit = (row >= 0) & (row < TERMS * H) & (row % H == head)
    return jnp.where(hit, -1.0, 0.0).astype(jnp.bfloat16)


def pair_kernel(
    off_ref, q_ref, do_ref, aux_ref, kv_ref, ds_ref, term_ref, keys_ref,
    flat_ref, bias_ref, dk_ref, dv_ref,
):
    step = pl.program_id(0)
    per_group = GROUP // STEP_HEADS
    c = step // per_group
    at = step % per_group
    rows = q_ref.shape[0]
    depth = kv_ref.shape[1]
    pieces = DH // depth

    @pl.when(step == 0)
    def _():
        flat_ref[...] = kv_ref[...].reshape(flat_ref.shape)
        keys_ref[...] = flat_ref[: KVH * DH, :]
        limit = lax.broadcasted_iota(jnp.int32, (rows, rows), 0) + off_ref[0]
        col = lax.broadcasted_iota(jnp.int32, (rows, rows), 1)
        bias_ref[...] = jnp.where(col <= limit, 0.0, -jnp.inf)

    @pl.when(at == 0)
    def _():
        dk_ref[...] = jnp.zeros_like(dk_ref)
        dv_ref[...] = jnp.zeros_like(dv_ref)

    k_t = flat_ref[pl.ds(pl.multiple_of(c * DH, DH), DH), :]
    v_t = flat_ref[pl.ds(pl.multiple_of((KVH + c) * DH, DH), DH), :]
    aux = aux_ref[...]

    def shifted(left, right, which, head):
        tail = jnp.concatenate([picker(which, head)] * (rows // DH), axis=1)
        return jnp.dot(
            jnp.concatenate([left, aux], axis=1),
            jnp.concatenate([right, tail], axis=0),
            preferred_element_type=jnp.float32,
        )

    for sub in range(STEP_HEADS):
        cols = slice(sub * DH, (sub + 1) * DH)
        head = step * STEP_HEADS + sub
        s = shifted(q_ref[:, cols], k_t, 0, head)
        dp = shifted(do_ref[:, cols], v_t, 1, head)
        p = jnp.exp2(s * (DH**-0.5 * LOG2E) + bias_ref[...])
        ds = (p * dp).astype(jnp.bfloat16)
        ds_ref[sub] = ds
        dv_ref[...] += jnp.dot(
            do_ref[:, cols].T, p.astype(jnp.bfloat16), preferred_element_type=jnp.float32
        )
        dk_ref[...] += jnp.dot(q_ref[:, cols].T, ds, preferred_element_type=jnp.float32)

    @pl.when(at == per_group - 1)
    def _():
        low_k = (dk_ref[...] * SCALE).astype(term_ref.dtype)
        low_v = dv_ref[...].astype(term_ref.dtype)
        term_ref[pl.ds(c * pieces, pieces)] = low_k.reshape(pieces, depth, rows)
        term_ref[pl.ds((KVH + c) * pieces, pieces)] = low_v.reshape(pieces, depth, rows)


def query_kernel(ds_ref, keys_ref, dq_ref, k_ref):
    step = pl.program_id(0)
    per_group = GROUP // STEP_HEADS
    c = step // per_group

    @pl.when(step % per_group == 0)
    def _():
        k_ref[...] = keys_ref[pl.ds(pl.multiple_of(c * DH, DH), DH), :].T

    for sub in range(STEP_HEADS):
        dq = jnp.dot(ds_ref[sub], k_ref[...], preferred_element_type=jnp.float32) * SCALE
        dq_ref[:, sub * DH : (sub + 1) * DH] = dq.astype(dq_ref.dtype)


def exchange(x):
    return lax.all_to_all(x, AXES, split_axis=0, concat_axis=0, tiled=True)


def cost(flops, bytes_accessed):
    return pl.CostEstimate(flops=flops, bytes_accessed=bytes_accessed, transcendentals=0)


def per_device(queries, key_rows, value_rows, out_grad, attn_out, log_norm, held_block, key_block):
    count = lax.axis_size("grp") * lax.axis_size("blk")
    own = lax.axis_index("grp") * lax.axis_size("blk") + lax.axis_index("blk")
    rows = queries.shape[0]
    depth = 2 * KVH * DH // count
    piece = (count, depth, rows)
    low = jax.ShapeDtypeStruct(piece, jnp.bfloat16)
    vmem = pl.BlockSpec(memory_space=pltpu.VMEM)
    smem = pl.BlockSpec(memory_space=pltpu.SMEM)
    hbm = pl.BlockSpec(memory_space=pltpu.HBM)
    width = STEP_HEADS * DH
    steps = H // STEP_HEADS
    wide = pl.BlockSpec((rows, width), lambda s: (0, s))
    keys_spec = pl.BlockSpec((KVH * DH, rows), lambda s: (0, 0))
    whole = pl.BlockSpec(piece, lambda s: (0, 0, 0))
    aux_spec = pl.BlockSpec((rows, DH), lambda s: (0, 0))
    big = pltpu.CompilerParams(
        dimension_semantics=("arbitrary",), vmem_limit_bytes=BIG_LIMIT
    )
    matmul = 2 * H * rows * rows * DH
    wide_bytes = 2 * rows * H * DH

    spread = pl.pallas_call(
        spread_kernel,
        out_shape=low,
        in_specs=[hbm] * 2,
        out_specs=vmem,
        scratch_shapes=[
            pltpu.VMEM(key_rows.shape, jnp.bfloat16),
            pltpu.VMEM(value_rows.shape, jnp.bfloat16),
            pltpu.SemaphoreType.DMA((2,)),
        ],
        compiler_params=pltpu.CompilerParams(vmem_limit_bytes=FULL_LIMIT),
        name="spread",
    )(key_rows, value_rows)
    gathered = exchange(spread)
    holder, off = pl.pallas_call(
        table_kernel,
        out_shape=(
            jax.ShapeDtypeStruct((count,), jnp.int32),
            jax.ShapeDtypeStruct((1,), jnp.int32),
        ),
        in_specs=[smem, smem, smem],
        out_specs=(smem, smem),
        scratch_shapes=[pltpu.SMEM((count,), jnp.int32)],
        compiler_params=SMALL,
        cost_estimate=cost(2**20, 2**12),
        name="table",
    )(own.reshape(1).astype(jnp.int32), held_block, key_block)
    aux = pl.pallas_call(
        prep_kernel,
        grid=(steps,),
        out_shape=jax.ShapeDtypeStruct((rows, DH), jnp.bfloat16),
        in_specs=[pl.BlockSpec(log_norm.shape, lambda s: (0, 0)), wide, wide],
        out_specs=aux_spec,
        scratch_shapes=[pltpu.VMEM((rows, DH), jnp.float32)],
        compiler_params=big,
        cost_estimate=cost(matmul // 2, 2 * wide_bytes),
        name="prep",
    )(log_norm, out_grad, attn_out)
    chosen = pl.pallas_call(
        select_kernel,
        out_shape=low,
        in_specs=[smem, vmem],
        out_specs=vmem,
        compiler_params=SMALL,
        name="select",
    )(holder, gathered)
    kv = exchange(chosen)

    kept = pl.BlockSpec((STEP_HEADS, rows, rows), lambda s: (s, 0, 0))
    ds, term, keys = pl.pallas_call(
        pair_kernel,
        grid=(steps,),
        out_shape=(
            jax.ShapeDtypeStruct((H, rows, rows), jnp.bfloat16),
            low,
            jax.ShapeDtypeStruct((KVH * DH, rows), jnp.bfloat16),
        ),
        in_specs=[smem, wide, wide, aux_spec, whole],
        out_specs=(kept, whole, keys_spec),
        scratch_shapes=[
            pltpu.VMEM((2 * KVH * DH, rows), jnp.bfloat16),
            pltpu.VMEM((rows, rows), jnp.float32),
            pltpu.VMEM((DH, rows), jnp.float32),
            pltpu.VMEM((DH, rows), jnp.float32),
        ],
        compiler_params=big,
        cost_estimate=cost(4 * matmul, 4 * wide_bytes + 2 * H * rows * rows),
        name="pair",
    )(off, queries, out_grad, aux, kv)
    returned = exchange(term)
    query_grad = pl.pallas_call(
        query_kernel,
        grid=(steps,),
        out_shape=jax.ShapeDtypeStruct(queries.shape, jnp.bfloat16),
        in_specs=[kept, keys_spec],
        out_specs=wide,
        scratch_shapes=[pltpu.VMEM((rows, DH), jnp.bfloat16)],
        compiler_params=big,
        cost_estimate=cost(matmul, wide_bytes + 2 * H * rows * rows),
        name="query",
    )(ds, keys)
    returned, query_grad = lax.optimization_barrier((returned, query_grad))
    pooled = pl.pallas_call(
        pool_kernel,
        out_shape=low,
        in_specs=[smem, vmem],
        out_specs=vmem,
        scratch_shapes=[pltpu.VMEM(piece, jnp.float32)],
        compiler_params=SMALL,
        name="pool",
    )(holder, returned)
    home = exchange(pooled)
    key_grad, value_grad = pl.pallas_call(
        finish_kernel,
        out_shape=(
            jax.ShapeDtypeStruct(key_rows.shape, jnp.bfloat16),
            jax.ShapeDtypeStruct(value_rows.shape, jnp.bfloat16),
        ),
        in_specs=[vmem],
        out_specs=(vmem, vmem),
        compiler_params=SMALL,
        name="finish",
    )(home)
    return (query_grad, key_grad, value_grad)


def solution(mesh):
    rows = P(AXES, None)
    return jax.shard_map(
        per_device,
        mesh=mesh,
        in_specs=(rows,) * 6 + (P(), P()),
        out_specs=(rows, rows, rows),
        check_vma=False,
    )
```

```python
import functools

import jax
import jax.numpy as jnp
from jax import lax
from jax.experimental import pallas as pl
from jax.experimental.pallas import tpu as pltpu
from jax.sharding import PartitionSpec as P

H = 16
KVH = 2
DH = 128
GROUP = H // KVH
AXES = ("grp", "blk")
SCALE = DH ** (-0.5)
LOG2E = 1.4426950408889634
STEP_HEADS = 4
TERMS = 3
SMALL = pltpu.CompilerParams(vmem_limit_bytes=8 * 1024 * 1024)
BLOCK = 640
BIG_LIMIT = 125 * 512 * 1024
FULL_LIMIT = 67043328


def spread_kernel(k_hbm, v_hbm, out_ref, k_ref, v_ref, sems):
    parts, depth, rows = out_ref.shape
    half = parts // 2
    copies = [
        pltpu.make_async_copy(k_hbm, k_ref, sems.at[0]),
        pltpu.make_async_copy(v_hbm, v_ref, sems.at[1]),
    ]
    for copy in copies:
        copy.start()
    for at, ref in enumerate((k_ref, v_ref)):
        copies[at].wait()
        out_ref[at * half : (at + 1) * half] = ref[...].T.reshape(half, depth, rows)


def table_kernel(own_ref, held_ref, key_ref, holder_ref, off_ref, pos_ref):
    def put(e, carry):
        pos_ref[held_ref[e]] = e
        return carry

    def look(d, carry):
        holder_ref[d] = pos_ref[key_ref[d]]
        return carry

    count = held_ref.shape[0]
    lax.fori_loop(0, count, put, 0, unroll=8)
    lax.fori_loop(0, count, look, 0, unroll=8)
    own = own_ref[0]
    off_ref[0] = jnp.where(held_ref[own] == key_ref[own], 0, BLOCK)


def prep_kernel(
    norm_ref, do_ref, o_ref, aux_ref, delta_ref,
):
    step = pl.program_id(0)
    rows = do_ref.shape[0]

    @pl.when(step == 0)
    def _():
        delta_ref[...] = jnp.zeros_like(delta_ref)

    lanes = lax.broadcasted_iota(jnp.int32, delta_ref.shape, 1)
    delta = delta_ref[...]
    for sub in range(STEP_HEADS):
        cols = slice(sub * DH, (sub + 1) * DH)
        both = do_ref[:, cols].astype(jnp.float32) * o_ref[:, cols].astype(jnp.float32)
        one = jnp.sum(both, axis=1, keepdims=True)
        delta = jnp.where(lanes == step * STEP_HEADS + sub, one, delta)
    delta_ref[...] = delta

    @pl.when(step == pl.num_programs(0) - 1)
    def _():
        norms = norm_ref[...] * DH**0.5
        norms = jnp.concatenate([norms, jnp.zeros((rows, DH - H), jnp.float32)], axis=1)
        total = jnp.zeros((rows, DH), jnp.float32)
        for at, left in enumerate((norms, delta_ref[...])):
            for term in range(TERMS):
                part = left.astype(jnp.bfloat16).astype(jnp.float32)
                left = left - part
                shift = (at * TERMS + term) * H
                total = total + (pltpu.roll(part, shift, 1) if shift else part)
        aux_ref[...] = total.astype(aux_ref.dtype)


def select_kernel(holder_ref, in_ref, out_ref):
    def move(d, carry):
        out_ref[d] = in_ref[holder_ref[d]]
        return carry

    lax.fori_loop(0, holder_ref.shape[0], move, 0, unroll=8)


def pool_kernel(holder_ref, in_ref, out_ref, total_ref):
    total_ref[...] = jnp.zeros_like(total_ref)

    def add(d, carry):
        at = holder_ref[d]
        total_ref[at] = total_ref[at] + in_ref[d].astype(jnp.float32)
        return carry

    lax.fori_loop(0, holder_ref.shape[0], add, 0, unroll=8)
    out_ref[...] = total_ref[...].astype(out_ref.dtype)


def finish_kernel(in_ref, k_ref, v_ref):
    parts, depth, rows = in_ref.shape
    half = parts // 2
    for at, ref in enumerate((k_ref, v_ref)):
        flat = in_ref[at * half : (at + 1) * half].reshape(half * depth, rows)
        ref[...] = flat.T


def picker(which, head):
    row = lax.broadcasted_iota(jnp.int32, (DH, DH), 0) - which * TERMS * H
    hit = (row >= 0) & (row < TERMS * H) & (row % H == head)
    return jnp.where(hit, -1.0, 0.0).astype(jnp.bfloat16)


def pair_kernel(
    off_ref, q_ref, do_ref, aux_ref, kv_ref, ds_ref, term_ref, keys_ref,
    flat_ref, bias_ref, dk_ref, dv_ref, slot_ref, sems,
):
    step = pl.program_id(0)
    per_group = GROUP // STEP_HEADS
    c = step // per_group
    at = step % per_group
    rows = q_ref.shape[0]
    depth = kv_ref.shape[1]
    pieces = DH // depth

    @pl.when(step == 0)
    def _():
        flat_ref[...] = kv_ref[...].reshape(flat_ref.shape)
        keys_ref[...] = flat_ref[: KVH * DH, :]
        limit = lax.broadcasted_iota(jnp.int32, (rows, rows), 0) + off_ref[0]
        col = lax.broadcasted_iota(jnp.int32, (rows, rows), 1)
        bias_ref[...] = jnp.where(col <= limit, 0.0, -jnp.inf)

    @pl.when(at == 0)
    def _():
        dk_ref[...] = jnp.zeros_like(dk_ref)
        dv_ref[...] = jnp.zeros_like(dv_ref)

    parity = step % 2

    def write(sub, side):
        return pltpu.make_async_copy(
            slot_ref.at[side, sub], ds_ref.at[step * STEP_HEADS + sub], sems.at[side, sub]
        )

    @pl.when(step >= 2)
    def _():
        for sub in range(STEP_HEADS):
            write(sub, parity).wait()

    k_t = flat_ref[pl.ds(pl.multiple_of(c * DH, DH), DH), :]
    v_t = flat_ref[pl.ds(pl.multiple_of((KVH + c) * DH, DH), DH), :]
    aux = aux_ref[...]

    def shifted(left, right, which, head):
        tail = jnp.concatenate([picker(which, head)] * (rows // DH), axis=1)
        return jnp.dot(
            jnp.concatenate([left, aux], axis=1),
            jnp.concatenate([right, tail], axis=0),
            preferred_element_type=jnp.float32,
        )

    for sub in range(STEP_HEADS):
        cols = slice(sub * DH, (sub + 1) * DH)
        head = step * STEP_HEADS + sub
        s = shifted(q_ref[:, cols], k_t, 0, head)
        dp = shifted(do_ref[:, cols], v_t, 1, head)
        p = jnp.exp2(s * (DH**-0.5 * LOG2E) + bias_ref[...])
        ds = (p * dp).astype(jnp.bfloat16)
        slot_ref[parity, sub] = ds
        write(sub, parity).start()
        dv_ref[...] += jnp.dot(
            do_ref[:, cols].T, p.astype(jnp.bfloat16), preferred_element_type=jnp.float32
        )
        dk_ref[...] += jnp.dot(q_ref[:, cols].T, ds, preferred_element_type=jnp.float32)

    @pl.when(at == per_group - 1)
    def _():
        low_k = (dk_ref[...] * SCALE).astype(term_ref.dtype)
        low_v = dv_ref[...].astype(term_ref.dtype)
        term_ref[pl.ds(c * pieces, pieces)] = low_k.reshape(pieces, depth, rows)
        term_ref[pl.ds((KVH + c) * pieces, pieces)] = low_v.reshape(pieces, depth, rows)

    @pl.when(step == pl.num_programs(0) - 1)
    def _():
        for side in range(2):
            for sub in range(STEP_HEADS):
                write(sub, side).wait()


def query_kernel(ds_ref, keys_ref, dq_ref, k_ref):
    step = pl.program_id(0)
    per_group = GROUP // STEP_HEADS
    c = step // per_group

    @pl.when(step % per_group == 0)
    def _():
        k_ref[...] = keys_ref[pl.ds(pl.multiple_of(c * DH, DH), DH), :].T

    for sub in range(STEP_HEADS):
        dq = jnp.dot(ds_ref[sub], k_ref[...], preferred_element_type=jnp.float32) * SCALE
        dq_ref[:, sub * DH : (sub + 1) * DH] = dq.astype(dq_ref.dtype)


def exchange(x):
    return lax.all_to_all(x, AXES, split_axis=0, concat_axis=0, tiled=True)


def cost(flops, bytes_accessed):
    return pl.CostEstimate(flops=flops, bytes_accessed=bytes_accessed, transcendentals=0)


def per_device(queries, key_rows, value_rows, out_grad, attn_out, log_norm, held_block, key_block):
    count = lax.axis_size("grp") * lax.axis_size("blk")
    own = lax.axis_index("grp") * lax.axis_size("blk") + lax.axis_index("blk")
    rows = queries.shape[0]
    depth = 2 * KVH * DH // count
    piece = (count, depth, rows)
    low = jax.ShapeDtypeStruct(piece, jnp.bfloat16)
    vmem = pl.BlockSpec(memory_space=pltpu.VMEM)
    smem = pl.BlockSpec(memory_space=pltpu.SMEM)
    hbm = pl.BlockSpec(memory_space=pltpu.HBM)
    width = STEP_HEADS * DH
    steps = H // STEP_HEADS
    wide = pl.BlockSpec((rows, width), lambda s: (0, s))
    keys_spec = pl.BlockSpec((KVH * DH, rows), lambda s: (0, 0))
    whole = pl.BlockSpec(piece, lambda s: (0, 0, 0))
    aux_spec = pl.BlockSpec((rows, DH), lambda s: (0, 0))
    big = pltpu.CompilerParams(
        dimension_semantics=("arbitrary",), vmem_limit_bytes=BIG_LIMIT
    )
    matmul = 2 * H * rows * rows * DH
    wide_bytes = 2 * rows * H * DH

    spread = pl.pallas_call(
        spread_kernel,
        out_shape=low,
        in_specs=[hbm] * 2,
        out_specs=vmem,
        scratch_shapes=[
            pltpu.VMEM(key_rows.shape, jnp.bfloat16),
            pltpu.VMEM(value_rows.shape, jnp.bfloat16),
            pltpu.SemaphoreType.DMA((2,)),
        ],
        compiler_params=pltpu.CompilerParams(vmem_limit_bytes=FULL_LIMIT),
        name="spread",
    )(key_rows, value_rows)
    gathered = exchange(spread)
    holder, off = pl.pallas_call(
        table_kernel,
        out_shape=(
            jax.ShapeDtypeStruct((count,), jnp.int32),
            jax.ShapeDtypeStruct((1,), jnp.int32),
        ),
        in_specs=[smem, smem, smem],
        out_specs=(smem, smem),
        scratch_shapes=[pltpu.SMEM((count,), jnp.int32)],
        compiler_params=SMALL,
        cost_estimate=cost(2**20, 2**12),
        name="table",
    )(own.reshape(1).astype(jnp.int32), held_block, key_block)
    aux = pl.pallas_call(
        prep_kernel,
        grid=(steps,),
        out_shape=jax.ShapeDtypeStruct((rows, DH), jnp.bfloat16),
        in_specs=[pl.BlockSpec(log_norm.shape, lambda s: (0, 0)), wide, wide],
        out_specs=aux_spec,
        scratch_shapes=[pltpu.VMEM((rows, DH), jnp.float32)],
        compiler_params=big,
        cost_estimate=cost(matmul // 2, 2 * wide_bytes),
        name="prep",
    )(log_norm, out_grad, attn_out)
    chosen = pl.pallas_call(
        select_kernel,
        out_shape=low,
        in_specs=[smem, vmem],
        out_specs=vmem,
        compiler_params=SMALL,
        name="select",
    )(holder, gathered)
    kv = exchange(chosen)

    kept = pl.BlockSpec((STEP_HEADS, rows, rows), lambda s: (s, 0, 0))
    ds, term, keys = pl.pallas_call(
        pair_kernel,
        grid=(steps,),
        out_shape=(
            jax.ShapeDtypeStruct((H, rows, rows), jnp.bfloat16),
            low,
            jax.ShapeDtypeStruct((KVH * DH, rows), jnp.bfloat16),
        ),
        in_specs=[smem, wide, wide, aux_spec, whole],
        out_specs=(hbm, whole, keys_spec),
        scratch_shapes=[
            pltpu.VMEM((2 * KVH * DH, rows), jnp.bfloat16),
            pltpu.VMEM((rows, rows), jnp.float32),
            pltpu.VMEM((DH, rows), jnp.float32),
            pltpu.VMEM((DH, rows), jnp.float32),
            pltpu.VMEM((2, STEP_HEADS, rows, rows), jnp.bfloat16),
            pltpu.SemaphoreType.DMA((2, STEP_HEADS)),
        ],
        compiler_params=big,
        cost_estimate=cost(4 * matmul, 4 * wide_bytes + 2 * H * rows * rows),
        name="pair",
    )(off, queries, out_grad, aux, kv)
    returned = exchange(term)
    query_grad = pl.pallas_call(
        query_kernel,
        grid=(steps,),
        out_shape=jax.ShapeDtypeStruct(queries.shape, jnp.bfloat16),
        in_specs=[kept, keys_spec],
        out_specs=wide,
        scratch_shapes=[pltpu.VMEM((rows, DH), jnp.bfloat16)],
        compiler_params=big,
        cost_estimate=cost(matmul, wide_bytes + 2 * H * rows * rows),
        name="query",
    )(ds, keys)
    returned, query_grad = lax.optimization_barrier((returned, query_grad))
    pooled = pl.pallas_call(
        pool_kernel,
        out_shape=low,
        in_specs=[smem, vmem],
        out_specs=vmem,
        scratch_shapes=[pltpu.VMEM(piece, jnp.float32)],
        compiler_params=SMALL,
        name="pool",
    )(holder, returned)
    home = exchange(pooled)
    key_grad, value_grad = pl.pallas_call(
        finish_kernel,
        out_shape=(
            jax.ShapeDtypeStruct(key_rows.shape, jnp.bfloat16),
            jax.ShapeDtypeStruct(value_rows.shape, jnp.bfloat16),
        ),
        in_specs=[vmem],
        out_specs=(vmem, vmem),
        compiler_params=SMALL,
        name="finish",
    )(home)
    return (query_grad, key_grad, value_grad)


def solution(mesh):
    rows = P(AXES, None)
    return jax.shard_map(
        per_device,
        mesh=mesh,
        in_specs=(rows,) * 6 + (P(), P()),
        out_specs=(rows, rows, rows),
        check_vma=False,
    )
```
